32 devices in a mesh: rows: 4 (over x, core), cols: 4 (over z), slabs: 2 (over y).
Axes of the slice: x: 2, y: 2, z: 4, core: 2. Of those that a mesh axis runs over, the one named last changes fastest.
Arguments:
- pressure: float32 [64, 32, 256, 128], P('rows', 'cols', 'slabs'), may hold values from 0.2 to 1.8
- earlier: float32 [64, 32, 256, 128], P('rows', 'cols', 'slabs'), may hold values from 0.2 to 1.8
- speed_square: float32 [64, 32, 256, 128], P('rows', 'cols', 'slabs'), may hold values from 0.05 to 0.3
Outputs:
- column_sum: float32 [64, 32, 256, 128], P('rows', 'cols', 'slabs')
- pressure_end: float32 [64, 32, 256, 128], P('rows', 'cols', 'slabs')
The draws below stay inside these ranges and needn't reach their ends.
All inputs are finite; a program needn't handle non-finite values.
Results may differ from the reference program's by a relative error of at most 0.00002.
Values sent between devices are 32-bit elements; how exact they have to be, the bound alone decides.
A program may use at most 128 MiB of HBM per device.

```python
import jax
import jax.numpy as jnp
from jax import lax

GRID_Y = 64
GRID_X = 32
GRID_Z = 256
MEMBERS = 128
STEPS = 6


def block_scale(key, extent, pieces, low, largest):
    factor_of = 1.0
    for dim, shards_of in pieces:
        steps = jax.random.uniform(jax.random.fold_in(jax.random.fold_in(key, 6), dim), (shards_of,), jnp.float32, low / len(pieces), largest / len(pieces))
        factor_of = factor_of * jnp.repeat(jnp.exp(steps), extent[dim] // shards_of).reshape((-1,) + (1,) * (len(extent) - 1 - dim))
    return factor_of


def setup_inputs(seed: int = 0) -> dict:
    arg_keys = jax.random.split(jax.random.key(seed), 4)
    pressure = jnp.clip(0.2 + 1.5999999 * jax.random.uniform(arg_keys[0], (GRID_Y, GRID_X, GRID_Z, MEMBERS), jnp.float32) ** block_scale(arg_keys[0], (GRID_Y, GRID_X, GRID_Z, MEMBERS), ((0, 4), (1, 4), (2, 2)), -0.2, 0.2), 0.2, 1.8)
    earlier = jnp.clip(0.2 + 1.5999999 * jax.random.uniform(arg_keys[1], (GRID_Y, GRID_X, GRID_Z, MEMBERS), jnp.float32) ** block_scale(arg_keys[1], (GRID_Y, GRID_X, GRID_Z, MEMBERS), ((0, 4), (1, 4), (2, 2)), -0.2, 0.2), 0.2, 1.8)
    speed_square = jnp.clip(0.05 + 0.25 * jax.random.uniform(arg_keys[2], (GRID_Y, GRID_X, GRID_Z, MEMBERS), jnp.float32) ** block_scale(arg_keys[2], (GRID_Y, GRID_X, GRID_Z, MEMBERS), ((0, 4), (1, 4), (2, 2)), -0.2, 0.2), 0.05, 0.3)
    return dict(pressure=pressure, earlier=earlier, speed_square=speed_square)


def inner_cells(values, dims):
    for dim in dims:
        values = lax.slice_in_dim(values, 1, values.shape[dim] - 1, axis=dim)
    return values


def side_cells(values, dim, start, dims):
    others = [other for other in dims if other != dim]
    values = inner_cells(values, others)
    return lax.slice_in_dim(values, start, start + values.shape[dim] - 2, axis=dim)


def advance(padded, before, speed_square):
    middle = inner_cells(padded, (0, 1, 2))
    lower = [side_cells(padded, dim, 0, (0, 1, 2)) for dim in (0, 1, 2)]
    upper = [side_cells(padded, dim, 2, (0, 1, 2)) for dim in (0, 1, 2)]
    spread = lower[0] + upper[0] + lower[1] + upper[1] + lower[2] + upper[2] - 6.0 * middle
    return 2.0 * middle - before + speed_square * spread


def reference(pressure, earlier, speed_square):
    for step in range(STEPS):
        later = advance(jnp.pad(pressure, ((1, 1), (1, 1), (1, 1), (0, 0)), mode="constant"), earlier, speed_square)
        earlier, pressure = pressure, later
    column_sum = jnp.cumsum(pressure, axis=1) / GRID_X
    return column_sum, pressure
```

```python
import functools

import jax
import jax.numpy as jnp
from jax import lax
from jax.experimental import pallas as pl
from jax.experimental.pallas import tpu as pltpu
from jax.sharding import PartitionSpec as P

STEPS = 6
PAD = 8
MESH = pl.DeviceIdType.MESH
AXES = ("rows", "cols", "slabs")


def kernel(counts, block, p_hbm, e_hbm, c_hbm, sum_hbm, end_hbm, field, speed, z_out, z_in, sum_in, sum_out,
           load_sem, x_send, x_recv, y_send, y_recv, z_send, z_recv, s_send, s_recv, store_sem):
    ny, nx, nz, _ = block
    chunk = 32 if nz % 32 == 0 else 8
    me = [lax.axis_index(axis) for axis in AXES]
    has = [(me[d] > 0, me[d] < counts[d] - 1) for d in range(3)]

    def other(d, side):
        return {AXES[d]: me[d] + (1 if side else -1)}

    def each(d):
        for side in (0, 1):
            if counts[d] > 1:
                yield side, has[d][side]

    core_z = pl.ds(PAD, nz)

    def load(which, y):
        hbm = (p_hbm, e_hbm, c_hbm)[which]
        dst = speed.at[y] if which == 2 else field.at[which, y + 1, pl.ds(1, nx), core_z, :]
        return pltpu.make_async_copy(hbm.at[y], dst, load_sem.at[which, y])

    def order(i):
        return (i + ny - 1) % ny

    def loads(i, _, which):
        for w in which:
            load(w, order(i)).start()
        return 0

    lax.fori_loop(0, ny, functools.partial(loads, which=(0,)), 0)
    lax.fori_loop(0, ny, functools.partial(loads, which=(1, 2)), 0)

    def x_copy(par, y, side, first=False):
        cell = nx - 1 if side else 0
        src = p_hbm.at[y, cell] if first else field.at[par, y + 1, cell + 1, core_z, :]
        return pltpu.make_async_remote_copy(
            src_ref=src,
            dst_ref=field.at[par, y + 1, 0 if side else nx + 1, core_z, :],
            send_sem=x_send.at[par, side, y], recv_sem=x_recv.at[par, 1 - side, y],
            device_id=other(1, side), device_id_type=MESH)

    def x_wait(par, y, side):
        here = field.at[par, y + 1, nx + 1 if side else 0, core_z, :]
        return pltpu.make_async_remote_copy(
            src_ref=here, dst_ref=here,
            send_sem=x_send.at[par, side, y], recv_sem=x_recv.at[par, side, y],
            device_id=other(1, side), device_id_type=MESH)

    def y_copy(par, side, first=False):
        cell = ny - 1 if side else 0
        src = p_hbm.at[cell] if first else field.at[par, cell + 1, pl.ds(1, nx), core_z, :]
        return pltpu.make_async_remote_copy(
            src_ref=src,
            dst_ref=field.at[par, 0 if side else ny + 1, pl.ds(1, nx), core_z, :],
            send_sem=y_send.at[par, side], recv_sem=y_recv.at[par, 1 - side],
            device_id=other(0, side), device_id_type=MESH)

    def y_wait(par, side):
        here = field.at[par, ny + 1 if side else 0, pl.ds(1, nx), core_z, :]
        return pltpu.make_async_remote_copy(
            src_ref=here, dst_ref=here,
            send_sem=y_send.at[par, side], recv_sem=y_recv.at[par, side],
            device_id=other(0, side), device_id_type=MESH)

    def z_copy(par, y, side):
        return pltpu.make_async_remote_copy(
            src_ref=z_out.at[par, side, y], dst_ref=z_in.at[par, 1 - side, y],
            send_sem=z_send.at[par, side, y], recv_sem=z_recv.at[par, 1 - side, y],
            device_id=other(2, side), device_id_type=MESH)

    def z_wait(par, y, side):
        here = z_in.at[par, side, y]
        return pltpu.make_async_remote_copy(
            src_ref=here, dst_ref=here,
            send_sem=z_send.at[par, side, y], recv_sem=z_recv.at[par, side, y],
            device_id=other(2, side), device_id_type=MESH)

    def s_copy(y):
        return pltpu.make_async_remote_copy(
            src_ref=sum_out.at[y], dst_ref=sum_in.at[y],
            send_sem=s_send.at[y], recv_sem=s_recv.at[y],
            device_id=other(1, 1), device_id_type=MESH)

    def s_wait(y):
        return pltpu.make_async_remote_copy(
            src_ref=sum_in.at[y], dst_ref=sum_in.at[y],
            send_sem=s_send.at[y], recv_sem=s_recv.at[y],
            device_id=other(1, 0), device_id_type=MESH)

    barrier = pltpu.get_barrier_semaphore()
    for d in range(3):
        for side, there in each(d):
            @pl.when(there)
            def _():
                pl.semaphore_signal(barrier, inc=1, device_id=other(d, side), device_id_type=MESH)
    peers = sum(there.astype(jnp.int32) for d in range(3) for _, there in each(d))
    pl.semaphore_wait(barrier, peers)

    for side, there in each(0):
        @pl.when(there)
        def _():
            y_copy(0, side, True).start()
    def first_x(i, _):
        for side, there in each(1):
            @pl.when(there)
            def _():
                x_copy(0, order(i), side, True).start()
        return 0
    lax.fori_loop(0, ny, first_x, 0)

    lanes = block[3]
    def zero_x(side):
        def body(y, _):
            for par in (0, 1):
                field[par, y + 1, nx + 1 if side else 0, core_z, :] = jnp.zeros((nz, lanes), jnp.float32)
            return 0
        lax.fori_loop(0, ny, body, 0)
    def zero_y(side):
        def body(x, _):
            for par in (0, 1):
                field[par, ny + 1 if side else 0, x + 1, core_z, :] = jnp.zeros((nz, lanes), jnp.float32)
            return 0
        lax.fori_loop(0, nx, body, 0)
    def zero_z(side):
        def body(y, _):
            for par in (0, 1):
                for x in range(nx):
                    field[par, y + 1, x + 1, pl.ds(PAD + nz if side else 0, PAD), :] = jnp.zeros((PAD, lanes), jnp.float32)
            return 0
        lax.fori_loop(0, ny, body, 0)
    def zero_s(y, _):
        sum_in[y] = jnp.zeros((nz, lanes), jnp.float32)
        return 0
    for d, zero in ((0, zero_y), (1, zero_x), (2, zero_z)):
        for side in (0, 1):
            pl.when(jnp.logical_not(has[d][side]))(functools.partial(zero, side))
    @pl.when(jnp.logical_not(has[1][0]))
    def _():
        lax.fori_loop(0, ny, zero_s, 0)

    def send_z(par, y):
        for side, there in each(2):
            @pl.when(there)
            def _():
                row = PAD + nz - 1 if side else PAD
                for x in range(nx):
                    z_out[par, side, y, pl.ds(x, 1), :] = field[par, y + 1, x + 1, pl.ds(row, 1), :]
                z_copy(par, y, side).start()

    def first_z(i, _):
        y = order(i)
        load(0, y).wait()
        send_z(0, y)
        return 0
    lax.fori_loop(0, ny, first_z, 0)

    def arrive(par, y):
        for side, there in each(1):
            @pl.when(there)
            def _():
                x_wait(par, y, side).wait_recv()
        for side, there in each(0):
            @pl.when(jnp.logical_and(there, y == (ny - 1 if side else 0)))
            def _():
                y_wait(par, side).wait_recv()
        for side, there in each(2):
            @pl.when(there)
            def _():
                z_wait(par, y, side).wait_recv()
                row = PAD + nz if side else PAD - 1
                for x in range(nx):
                    field[par, y + 1, x + 1, pl.ds(row, 1), :] = z_in[par, side, y, pl.ds(x, 1), :]

    def sent(par, y):
        for side, there in each(1):
            @pl.when(there)
            def _():
                x_copy(par, y, side).wait_send()
        for side, there in each(0):
            @pl.when(jnp.logical_and(there, y == (ny - 1 if side else 0)))
            def _():
                y_copy(par, side).wait_send()
        for side, there in each(2):
            @pl.when(there)
            def _():
                z_copy(par, y, side).wait_send()

    def cell(par, y, x, z):
        def at(dy, dx, dz):
            return field[par, y + 1 + dy, x + 1 + dx, pl.ds(PAD + z + dz, chunk), :]
        middle = at(0, 0, 0)
        spread = (at(-1, 0, 0) + at(1, 0, 0) + at(0, -1, 0) + at(0, 1, 0) + at(0, 0, -1) + at(0, 0, 1)
                  - 6.0 * middle)
        before = field[1 - par, y + 1, x + 1, pl.ds(PAD + z, chunk), :]
        later = 2.0 * middle - before + speed[y, x, pl.ds(z, chunk), :] * spread
        field[1 - par, y + 1, x + 1, pl.ds(PAD + z, chunk), :] = later
        return later

    def step(t, _):
        par = t % 2
        def row(i, _):
            y = order(i)
            @pl.when(t == 0)
            def _():
                load(1, y).wait()
                load(2, y).wait()
            arrive(par, y)
            @pl.when(t > 0)
            def _():
                sent(1 - par, y)
            def along(x, _):
                for z in range(0, nz, chunk):
                    cell(par, y, x, z)
                return 0
            lax.fori_loop(0, nx, along, 0)
            for side, there in each(1):
                @pl.when(there)
                def _():
                    x_copy(1 - par, y, side).start()
            for side, there in each(0):
                @pl.when(jnp.logical_and(there, y == (ny - 1 if side else 0)))
                def _():
                    y_copy(1 - par, side).start()
            send_z(1 - par, y)
            return 0
        lax.fori_loop(0, ny, row, 0)
        return 0
    lax.fori_loop(0, STEPS - 1, step, 0)

    last = (STEPS - 1) % 2

    def end_copy(y):
        return pltpu.make_async_copy(field.at[1 - last, y + 1, pl.ds(1, nx), core_z, :], end_hbm.at[y], store_sem.at[0, y])

    def sum_copy(y):
        return pltpu.make_async_copy(speed.at[y], sum_hbm.at[y], store_sem.at[1, y])

    def last_row(i, _):
        y = order(i)
        arrive(last, y)
        sent(1 - last, y)
        for z in range(0, nz, chunk):
            def along(x, total):
                total = total + cell(last, y, x, z)
                speed[y, x, pl.ds(z, chunk), :] = total
                return total
            total = lax.fori_loop(0, nx, along, jnp.zeros((chunk, lanes), jnp.float32))
            @pl.when(jnp.logical_not(has[1][0]))
            def _():
                sum_out[y, pl.ds(z, chunk), :] = total
        if counts[1] > 1:
            @pl.when(jnp.logical_not(has[1][0]))
            def _():
                s_copy(y).start()
        end_copy(y).start()
        return 0
    lax.fori_loop(0, ny, last_row, 0)

    scale = 1.0 / (nx * counts[1])

    def finish(i, _):
        y = order(i)
        if counts[1] > 1:
            @pl.when(has[1][0])
            def _():
                s_wait(y).wait_recv()
                @pl.when(has[1][1])
                def _():
                    for z in range(0, nz, chunk):
                        at = pl.ds(z, chunk)
                        sum_out[y, at, :] = sum_in[y, at, :] + speed[y, nx - 1, at, :]
                    s_copy(y).start()
        for z in range(0, nz, chunk):
            at = pl.ds(z, chunk)
            below = sum_in[y, at, :]
            def along(x, _):
                speed[y, x, at, :] = (speed[y, x, at, :] + below) * scale
                return 0
            lax.fori_loop(0, nx, along, 0)
        sum_copy(y).start()
        return 0
    lax.fori_loop(0, ny, finish, 0)

    def drain(i, _):
        y = order(i)
        sent(last, y)
        if counts[1] > 1:
            @pl.when(has[1][1])
            def _():
                s_copy(y).wait_send()
        end_copy(y).wait()
        sum_copy(y).wait()
        return 0
    lax.fori_loop(0, ny, drain, 0)


def solution(mesh):
    counts = tuple(mesh.shape[axis] for axis in AXES)

    def on_device(pressure, earlier, speed_square):
        block = pressure.shape
        ny, nx, nz, lanes = block
        f32 = jnp.float32
        anywhere = pl.BlockSpec(memory_space=pl.ANY)
        dma = pltpu.SemaphoreType.DMA
        return pl.pallas_call(
            functools.partial(kernel, counts, block),
            out_shape=[jax.ShapeDtypeStruct(block, f32)] * 2,
            in_specs=[anywhere] * 3,
            out_specs=[anywhere] * 2,
            scratch_shapes=[
                pltpu.VMEM((2, ny + 2, nx + 2, nz + 2 * PAD, lanes), f32),
                pltpu.VMEM((ny, nx, nz, lanes), f32),
                pltpu.VMEM((2, 2, ny, nx, lanes), f32),
                pltpu.VMEM((2, 2, ny, nx, lanes), f32),
                pltpu.VMEM((ny, nz, lanes), f32),
                pltpu.VMEM((ny, nz, lanes), f32),
                dma((3, ny)),
                dma((2, 2, ny)), dma((2, 2, ny)),
                dma((2, 2)), dma((2, 2)),
                dma((2, 2, ny)), dma((2, 2, ny)),
                dma((ny,)), dma((ny,)),
                dma((2, ny)),
            ],
            compiler_params=pltpu.CompilerParams(
                collective_id=0, has_side_effects=True, vmem_limit_bytes=60 * 1024 * 1024
            ),
        )(pressure, earlier, speed_square)

    spec = P("rows", "cols", "slabs", None)
    return jax.shard_map(
        on_device, mesh=mesh, in_specs=(spec, spec, spec), out_specs=(spec, spec), check_vma=False
    )
```

```python
import functools

import jax
import jax.numpy as jnp
from jax import lax
from jax.experimental import pallas as pl
from jax.experimental.pallas import tpu as pltpu
from jax.sharding import PartitionSpec as P

STEPS = 6
PAD = 8
MESH = pl.DeviceIdType.MESH
AXES = ("rows", "cols", "slabs")


def kernel(counts, block, p_hbm, e_hbm, c_hbm, speed, end, field, z_out, z_in, sum_in, sum_out,
           load_sem, x_send, x_recv, y_send, y_recv, z_send, z_recv, s_send, s_recv):
    ny, nx, nz, _ = block
    parts = 2 if nz % (2 * PAD) == 0 else 1
    half = nz // parts
    chunk = 32 if half % 32 == 0 else PAD
    me = [lax.axis_index(axis) for axis in AXES]
    has = [(me[d] > 0, me[d] < counts[d] - 1) for d in range(3)]

    def other(d, side):
        return {AXES[d]: me[d] + (1 if side else -1)}

    def each(d):
        for side in (0, 1):
            if counts[d] > 1:
                yield side, has[d][side]

    core_z = pl.ds(PAD, nz)

    barrier = pltpu.get_barrier_semaphore()
    for d in range(3):
        for side, there in each(d):
            @pl.when(there)
            def _():
                pl.semaphore_signal(barrier, inc=1, device_id=other(d, side), device_id_type=MESH)

    def load(which, y):
        hbm = (p_hbm, e_hbm, c_hbm)[which]
        dst = speed.at[y] if which == 2 else field.at[which, y + 1, pl.ds(1, nx), core_z, :]
        return pltpu.make_async_copy(hbm.at[y], dst, load_sem.at[which, y])

    def order(i):
        return (i + ny - 1) % ny

    def loads(i, _, which):
        for w in which:
            load(w, order(i)).start()
        return 0

    def x_copy(par, y, side, first=False):
        cell = nx - 1 if side else 0
        src = p_hbm.at[y, cell] if first else field.at[par, y + 1, cell + 1, core_z, :]
        return pltpu.make_async_remote_copy(
            src_ref=src,
            dst_ref=field.at[par, y + 1, 0 if side else nx + 1, core_z, :],
            send_sem=x_send.at[par, side, y], recv_sem=x_recv.at[par, 1 - side, y],
            device_id=other(1, side), device_id_type=MESH)

    def x_wait(par, y, side):
        here = field.at[par, y + 1, nx + 1 if side else 0, core_z, :]
        return pltpu.make_async_remote_copy(
            src_ref=here, dst_ref=here,
            send_sem=x_send.at[par, side, y], recv_sem=x_recv.at[par, side, y],
            device_id=other(1, side), device_id_type=MESH)

    def y_copy(par, side, first=False):
        cell = ny - 1 if side else 0
        src = p_hbm.at[cell] if first else field.at[par, cell + 1, pl.ds(1, nx), core_z, :]
        return pltpu.make_async_remote_copy(
            src_ref=src,
            dst_ref=field.at[par, 0 if side else ny + 1, pl.ds(1, nx), core_z, :],
            send_sem=y_send.at[par, side], recv_sem=y_recv.at[par, 1 - side],
            device_id=other(0, side), device_id_type=MESH)

    def y_wait(par, side):
        here = field.at[par, ny + 1 if side else 0, pl.ds(1, nx), core_z, :]
        return pltpu.make_async_remote_copy(
            src_ref=here, dst_ref=here,
            send_sem=y_send.at[par, side], recv_sem=y_recv.at[par, side],
            device_id=other(0, side), device_id_type=MESH)

    def z_copy(par, y, side):
        return pltpu.make_async_remote_copy(
            src_ref=z_out.at[par, side, y], dst_ref=z_in.at[par, 1 - side, y],
            send_sem=z_send.at[par, side, y], recv_sem=z_recv.at[par, 1 - side, y],
            device_id=other(2, side), device_id_type=MESH)

    def z_wait(par, y, side):
        here = z_in.at[par, side, y]
        return pltpu.make_async_remote_copy(
            src_ref=here, dst_ref=here,
            send_sem=z_send.at[par, side, y], recv_sem=z_recv.at[par, side, y],
            device_id=other(2, side), device_id_type=MESH)

    def s_copy(y, part):
        at = pl.ds(pl.multiple_of(part * half, PAD), half)
        return pltpu.make_async_remote_copy(
            src_ref=sum_out.at[y, at, :], dst_ref=sum_in.at[y, at, :],
            send_sem=s_send.at[y, part], recv_sem=s_recv.at[y, part],
            device_id=other(1, 1), device_id_type=MESH)

    def s_wait(y, part):
        here = sum_in.at[y, pl.ds(pl.multiple_of(part * half, PAD), half), :]
        return pltpu.make_async_remote_copy(
            src_ref=here, dst_ref=here,
            send_sem=s_send.at[y, part], recv_sem=s_recv.at[y, part],
            device_id=other(1, 0), device_id_type=MESH)

    peers = sum(there.astype(jnp.int32) for d in range(3) for _, there in each(d))
    pl.semaphore_wait(barrier, peers)

    for side, there in each(0):
        @pl.when(there)
        def _():
            y_copy(0, side, True).start()
    def first_x(i, _):
        for side, there in each(1):
            @pl.when(there)
            def _():
                x_copy(0, order(i), side, True).start()
        return 0
    lax.fori_loop(0, ny, first_x, 0)
    lax.fori_loop(0, ny, functools.partial(loads, which=(0,)), 0)
    lax.fori_loop(0, ny, functools.partial(loads, which=(1, 2)), 0)

    lanes = block[3]
    def zero_x(side):
        def body(y, _):
            for par in (0, 1):
                field[par, y + 1, nx + 1 if side else 0, core_z, :] = jnp.zeros((nz, lanes), jnp.float32)
            return 0
        lax.fori_loop(0, ny, body, 0)
    def zero_y(side):
        def body(x, _):
            for par in (0, 1):
                field[par, ny + 1 if side else 0, x + 1, core_z, :] = jnp.zeros((nz, lanes), jnp.float32)
            return 0
        lax.fori_loop(0, nx, body, 0)
    def zero_z(side):
        def body(y, _):
            for par in (0, 1):
                for x in range(nx):
                    field[par, y + 1, x + 1, pl.ds(PAD + nz if side else 0, PAD), :] = jnp.zeros((PAD, lanes), jnp.float32)
            return 0
        lax.fori_loop(0, ny, body, 0)
    def zero_s(y, _):
        sum_in[y] = jnp.zeros((nz, lanes), jnp.float32)
        return 0
    for d, zero in ((0, zero_y), (1, zero_x), (2, zero_z)):
        for side in (0, 1):
            pl.when(jnp.logical_not(has[d][side]))(functools.partial(zero, side))
    @pl.when(jnp.logical_not(has[1][0]))
    def _():
        lax.fori_loop(0, ny, zero_s, 0)

    def send_z(par, y):
        for side, there in each(2):
            @pl.when(there)
            def _():
                row = PAD + nz - 1 if side else PAD
                for x in range(nx):
                    z_out[par, side, y, pl.ds(x, 1), :] = field[par, y + 1, x + 1, pl.ds(row, 1), :]
                z_copy(par, y, side).start()

    def first_z(i, _):
        y = order(i)
        load(0, y).wait()
        send_z(0, y)
        return 0
    lax.fori_loop(0, ny, first_z, 0)

    def arrive(par, y):
        for side, there in each(1):
            @pl.when(there)
            def _():
                x_wait(par, y, side).wait_recv()
        for side, there in each(0):
            @pl.when(jnp.logical_and(there, y == (ny - 1 if side else 0)))
            def _():
                y_wait(par, side).wait_recv()
        for side, there in each(2):
            @pl.when(there)
            def _():
                z_wait(par, y, side).wait_recv()
                row = PAD + nz if side else PAD - 1
                for x in range(nx):
                    field[par, y + 1, x + 1, pl.ds(row, 1), :] = z_in[par, side, y, pl.ds(x, 1), :]

    def sent(par, y):
        for side, there in each(1):
            @pl.when(there)
            def _():
                x_copy(par, y, side).wait_send()
        for side, there in each(0):
            @pl.when(jnp.logical_and(there, y == (ny - 1 if side else 0)))
            def _():
                y_copy(par, side).wait_send()
        for side, there in each(2):
            @pl.when(there)
            def _():
                z_copy(par, y, side).wait_send()

    def cell(par, y, x, z, final=False):
        def at(dy, dx, dz):
            return field[par, y + 1 + dy, x + 1 + dx, pl.ds(PAD + z + dz, chunk), :]
        middle = at(0, 0, 0)
        spread = (at(-1, 0, 0) + at(1, 0, 0) + at(0, -1, 0) + at(0, 1, 0) + at(0, 0, -1) + at(0, 0, 1)
                  - 6.0 * middle)
        before = field[1 - par, y + 1, x + 1, pl.ds(PAD + z, chunk), :]
        later = 2.0 * middle - before + speed[y, x, pl.ds(z, chunk), :] * spread
        if final:
            end[y, x, pl.ds(z, chunk), :] = later
        else:
            field[1 - par, y + 1, x + 1, pl.ds(PAD + z, chunk), :] = later
        return later

    def step(t, _):
        par = t % 2
        def row(i, _):
            y = order(i)
            @pl.when(t == 0)
            def _():
                load(1, y).wait()
                load(2, y).wait()
            arrive(par, y)
            @pl.when(t > 0)
            def _():
                sent(1 - par, y)
            def along(x, _):
                for z in range(0, nz, chunk):
                    cell(par, y, x, z)
                return 0
            lax.fori_loop(0, nx, along, 0)
            for side, there in each(1):
                @pl.when(there)
                def _():
                    x_copy(1 - par, y, side).start()
            for side, there in each(0):
                @pl.when(jnp.logical_and(there, y == (ny - 1 if side else 0)))
                def _():
                    y_copy(1 - par, side).start()
            send_z(1 - par, y)
            return 0
        lax.fori_loop(0, ny, row, 0)
        return 0
    lax.fori_loop(0, STEPS - 1, step, 0)

    last = (STEPS - 1) % 2

    def last_row(i, _):
        y = order(i)
        arrive(last, y)
        sent(1 - last, y)
        for z in range(0, nz, chunk):
            def along(x, total):
                total = total + cell(last, y, x, z, True)
                speed[y, x, pl.ds(z, chunk), :] = total
                return total
            total = lax.fori_loop(0, nx, along, jnp.zeros((chunk, lanes), jnp.float32))
            if counts[1] > 1:
                @pl.when(jnp.logical_not(has[1][0]))
                def _():
                    sum_out[y, pl.ds(z, chunk), :] = total
                    if (z + chunk) % half == 0:
                        s_copy(y, z // half).start()
        return 0
    lax.fori_loop(0, ny, last_row, 0)

    scale = 1.0 / (nx * counts[1])

    def finish(i, _):
        y, part = order(i // parts), i % parts
        places = [pl.ds(pl.multiple_of(part * half + z, PAD), chunk) for z in range(0, half, chunk)]
        if counts[1] > 1:
            @pl.when(has[1][0])
            def _():
                s_wait(y, part).wait_recv()
                @pl.when(has[1][1])
                def _():
                    for at in places:
                        sum_out[y, at, :] = sum_in[y, at, :] + speed[y, nx - 1, at, :]
                    s_copy(y, part).start()
        for at in places:
            below = sum_in[y, at, :]
            for x in range(nx):
                speed[y, x, at, :] = (speed[y, x, at, :] + below) * scale
        return 0
    lax.fori_loop(0, ny * parts, finish, 0)

    def drain(i, _):
        y = order(i)
        sent(last, y)
        if counts[1] > 1:
            @pl.when(has[1][1])
            def _():
                for part in range(parts):
                    s_copy(y, part).wait_send()
        return 0
    lax.fori_loop(0, ny, drain, 0)


def write(rows, sum_ref, end_ref, sum_hbm, end_hbm, sem):
    def copies(y):
        return (pltpu.make_async_copy(sum_ref.at[y], sum_hbm.at[y], sem.at[0, y]),
                pltpu.make_async_copy(end_ref.at[y], end_hbm.at[y], sem.at[1, y]))

    for y in range(rows):
        for copy in copies(y):
            copy.start()
    for y in range(rows):
        for copy in copies(y):
            copy.wait()


def solution(mesh):
    counts = tuple(mesh.shape[axis] for axis in AXES)

    def on_device(pressure, earlier, speed_square):
        block = pressure.shape
        ny, nx, nz, lanes = block
        f32 = jnp.float32
        anywhere = pl.BlockSpec(memory_space=pl.ANY)
        inside = pl.BlockSpec(memory_space=pltpu.VMEM)
        dma = pltpu.SemaphoreType.DMA
        column_sum, pressure_end = pl.pallas_call(
            functools.partial(kernel, counts, block),
            out_shape=[pltpu.VMEM(block, f32)] * 2,
            in_specs=[anywhere] * 3,
            out_specs=[inside] * 2,
            scratch_shapes=[
                pltpu.VMEM((2, ny + 2, nx + 2, nz + 2 * PAD, lanes), f32),
                pltpu.VMEM((2, 2, ny, nx, lanes), f32),
                pltpu.VMEM((2, 2, ny, nx, lanes), f32),
                pltpu.VMEM((ny, nz, lanes), f32),
                pltpu.VMEM((ny, nz, lanes), f32),
                dma((3, ny)),
                dma((2, 2, ny)), dma((2, 2, ny)),
                dma((2, 2)), dma((2, 2)),
                dma((2, 2, ny)), dma((2, 2, ny)),
                dma((ny, 2)), dma((ny, 2)),
            ],
            compiler_params=pltpu.CompilerParams(
                collective_id=0, has_side_effects=True, vmem_limit_bytes=40 * 1024 * 1024
            ),
        )(pressure, earlier, speed_square)
        return pl.pallas_call(
            functools.partial(write, ny),
            out_shape=[jax.ShapeDtypeStruct(block, f32)] * 2,
            in_specs=[inside] * 2,
            out_specs=[anywhere] * 2,
            scratch_shapes=[dma((2, ny))],
            compiler_params=pltpu.CompilerParams(vmem_limit_bytes=1024 * 1024),
        )(column_sum, pressure_end)

    spec = P("rows", "cols", "slabs", None)
    return jax.shard_map(
        on_device, mesh=mesh, in_specs=(spec, spec, spec), out_specs=(spec, spec), check_vma=False
    )
```

```python
import functools

import jax
import jax.numpy as jnp
from jax import lax
from jax.experimental import pallas as pl
from jax.experimental.pallas import tpu as pltpu
from jax.sharding import PartitionSpec as P

STEPS = 6
PAD = 8
MESH = pl.DeviceIdType.MESH
AXES = ("rows", "cols", "slabs")


def pieces(nz):
    return 4 if nz % (4 * PAD) == 0 else 1


def kernel(counts, block, p_hbm, e_hbm, c_hbm, speed, end, field, z_out, z_in, sum_in, sum_out,
           load_sem, x_send, x_recv, y_send, y_recv, z_send, z_recv, s_send, s_recv):
    ny, nx, nz, _ = block
    parts = pieces(nz)
    half = nz // parts
    chunk = 32 if half % 32 == 0 else PAD
    me = [lax.axis_index(axis) for axis in AXES]
    has = [(me[d] > 0, me[d] < counts[d] - 1) for d in range(3)]

    def other(d, side):
        return {AXES[d]: me[d] + (1 if side else -1)}

    def each(d):
        for side in (0, 1):
            if counts[d] > 1:
                yield side, has[d][side]

    core_z = pl.ds(PAD, nz)

    barrier = pltpu.get_barrier_semaphore()
    for d in range(3):
        for side, there in each(d):
            @pl.when(there)
            def _():
                pl.semaphore_signal(barrier, inc=1, device_id=other(d, side), device_id_type=MESH)

    def load(which, y):
        hbm = (p_hbm, e_hbm, c_hbm)[which]
        dst = speed.at[y] if which == 2 else field.at[which, y + 1, pl.ds(1, nx), core_z, :]
        return pltpu.make_async_copy(hbm.at[y], dst, load_sem.at[which, y])

    def order(i):
        return (i + ny - 1) % ny

    def loads(i, _, which):
        for w in which:
            load(w, order(i)).start()
        return 0

    def x_copy(par, y, side, first=False):
        cell = nx - 1 if side else 0
        src = p_hbm.at[y, cell] if first else field.at[par, y + 1, cell + 1, core_z, :]
        return pltpu.make_async_remote_copy(
            src_ref=src,
            dst_ref=field.at[par, y + 1, 0 if side else nx + 1, core_z, :],
            send_sem=x_send.at[par, side, y], recv_sem=x_recv.at[par, 1 - side, y],
            device_id=other(1, side), device_id_type=MESH)

    def x_wait(par, y, side):
        here = field.at[par, y + 1, nx + 1 if side else 0, core_z, :]
        return pltpu.make_async_remote_copy(
            src_ref=here, dst_ref=here,
            send_sem=x_send.at[par, side, y], recv_sem=x_recv.at[par, side, y],
            device_id=other(1, side), device_id_type=MESH)

    def y_copy(par, side, first=False):
        cell = ny - 1 if side else 0
        src = p_hbm.at[cell] if first else field.at[par, cell + 1, pl.ds(1, nx), core_z, :]
        return pltpu.make_async_remote_copy(
            src_ref=src,
            dst_ref=field.at[par, 0 if side else ny + 1, pl.ds(1, nx), core_z, :],
            send_sem=y_send.at[par, side], recv_sem=y_recv.at[par, 1 - side],
            device_id=other(0, side), device_id_type=MESH)

    def y_wait(par, side):
        here = field.at[par, ny + 1 if side else 0, pl.ds(1, nx), core_z, :]
        return pltpu.make_async_remote_copy(
            src_ref=here, dst_ref=here,
            send_sem=y_send.at[par, side], recv_sem=y_recv.at[par, side],
            device_id=other(0, side), device_id_type=MESH)

    def z_copy(par, y, side):
        return pltpu.make_async_remote_copy(
            src_ref=z_out.at[par, side, y], dst_ref=z_in.at[par, 1 - side, y],
            send_sem=z_send.at[par, side, y], recv_sem=z_recv.at[par, 1 - side, y],
            device_id=other(2, side), device_id_type=MESH)

    def z_wait(par, y, side):
        here = z_in.at[par, side, y]
        return pltpu.make_async_remote_copy(
            src_ref=here, dst_ref=here,
            send_sem=z_send.at[par, side, y], recv_sem=z_recv.at[par, side, y],
            device_id=other(2, side), device_id_type=MESH)

    def s_copy(y, part):
        at = pl.ds(pl.multiple_of(part * half, PAD), half)
        return pltpu.make_async_remote_copy(
            src_ref=sum_out.at[y, at, :], dst_ref=sum_in.at[y, at, :],
            send_sem=s_send.at[y, part], recv_sem=s_recv.at[y, part],
            device_id=other(1, 1), device_id_type=MESH)

    def s_wait(y, part):
        here = sum_in.at[y, pl.ds(pl.multiple_of(part * half, PAD), half), :]
        return pltpu.make_async_remote_copy(
            src_ref=here, dst_ref=here,
            send_sem=s_send.at[y, part], recv_sem=s_recv.at[y, part],
            device_id=other(1, 0), device_id_type=MESH)

    peers = sum(there.astype(jnp.int32) for d in range(3) for _, there in each(d))
    pl.semaphore_wait(barrier, peers)

    for side, there in each(0):
        @pl.when(there)
        def _():
            y_copy(0, side, True).start()
    def first_x(i, _):
        for side, there in each(1):
            @pl.when(there)
            def _():
                x_copy(0, order(i), side, True).start()
        return 0
    lax.fori_loop(0, ny, first_x, 0)
    lax.fori_loop(0, ny, functools.partial(loads, which=(0,)), 0)
    lax.fori_loop(0, ny, functools.partial(loads, which=(1, 2)), 0)

    lanes = block[3]
    def zero_x(side):
        def body(y, _):
            for par in (0, 1):
                field[par, y + 1, nx + 1 if side else 0, core_z, :] = jnp.zeros((nz, lanes), jnp.float32)
            return 0
        lax.fori_loop(0, ny, body, 0)
    def zero_y(side):
        def body(x, _):
            for par in (0, 1):
                field[par, ny + 1 if side else 0, x + 1, core_z, :] = jnp.zeros((nz, lanes), jnp.float32)
            return 0
        lax.fori_loop(0, nx, body, 0)
    def zero_z(side):
        def body(y, _):
            for par in (0, 1):
                for x in range(nx):
                    field[par, y + 1, x + 1, pl.ds(PAD + nz if side else 0, PAD), :] = jnp.zeros((PAD, lanes), jnp.float32)
            return 0
        lax.fori_loop(0, ny, body, 0)
    def zero_s(y, _):
        sum_in[y] = jnp.zeros((nz, lanes), jnp.float32)
        return 0
    for d, zero in ((0, zero_y), (1, zero_x), (2, zero_z)):
        for side in (0, 1):
            pl.when(jnp.logical_not(has[d][side]))(functools.partial(zero, side))
    @pl.when(jnp.logical_not(has[1][0]))
    def _():
        lax.fori_loop(0, ny, zero_s, 0)

    def send_z(par, y):
        for side, there in each(2):
            @pl.when(there)
            def _():
                row = PAD + nz - 1 if side else PAD
                for x in range(nx):
                    z_out[par, side, y, pl.ds(x, 1), :] = field[par, y + 1, x + 1, pl.ds(row, 1), :]
                z_copy(par, y, side).start()

    def first_z(i, _):
        y = order(i)
        load(0, y).wait()
        send_z(0, y)
        return 0
    lax.fori_loop(0, ny, first_z, 0)

    def arrive(par, y):
        for side, there in each(1):
            @pl.when(there)
            def _():
                x_wait(par, y, side).wait_recv()
        for side, there in each(0):
            @pl.when(jnp.logical_and(there, y == (ny - 1 if side else 0)))
            def _():
                y_wait(par, side).wait_recv()
        for side, there in each(2):
            @pl.when(there)
            def _():
                z_wait(par, y, side).wait_recv()
                row = PAD + nz if side else PAD - 1
                for x in range(nx):
                    field[par, y + 1, x + 1, pl.ds(row, 1), :] = z_in[par, side, y, pl.ds(x, 1), :]

    def sent(par, y):
        for side, there in each(1):
            @pl.when(there)
            def _():
                x_copy(par, y, side).wait_send()
        for side, there in each(0):
            @pl.when(jnp.logical_and(there, y == (ny - 1 if side else 0)))
            def _():
                y_copy(par, side).wait_send()
        for side, there in each(2):
            @pl.when(there)
            def _():
                z_copy(par, y, side).wait_send()

    def cell(par, y, x, z, final=False):
        def at(dy, dx, dz):
            return field[par, y + 1 + dy, x + 1 + dx, pl.ds(PAD + z + dz, chunk), :]
        middle = at(0, 0, 0)
        spread = (at(-1, 0, 0) + at(1, 0, 0) + at(0, -1, 0) + at(0, 1, 0) + at(0, 0, -1) + at(0, 0, 1)
                  - 6.0 * middle)
        before = field[1 - par, y + 1, x + 1, pl.ds(PAD + z, chunk), :]
        later = 2.0 * middle - before + speed[y, x, pl.ds(z, chunk), :] * spread
        if final:
            end[y, x, pl.ds(z, chunk), :] = later
        else:
            field[1 - par, y + 1, x + 1, pl.ds(PAD + z, chunk), :] = later
        return later

    def step(t, _):
        par = t % 2
        def row(i, _):
            y = order(i)
            @pl.when(t == 0)
            def _():
                load(1, y).wait()
                load(2, y).wait()
            arrive(par, y)
            @pl.when(t > 0)
            def _():
                sent(1 - par, y)
            def along(x, _):
                for z in range(0, nz, chunk):
                    cell(par, y, x, z)
                return 0
            lax.fori_loop(0, nx, along, 0)
            for side, there in each(1):
                @pl.when(there)
                def _():
                    x_copy(1 - par, y, side).start()
            for side, there in each(0):
                @pl.when(jnp.logical_and(there, y == (ny - 1 if side else 0)))
                def _():
                    y_copy(1 - par, side).start()
            send_z(1 - par, y)
            return 0
        lax.fori_loop(0, ny, row, 0)
        return 0
    lax.fori_loop(0, STEPS - 1, step, 0)

    last = (STEPS - 1) % 2

    def last_row(i, _):
        y = order(i)
        arrive(last, y)
        sent(1 - last, y)
        for z in range(0, nz, chunk):
            def along(x, total):
                total = total + cell(last, y, x, z, True)
                speed[y, x, pl.ds(z, chunk), :] = total
                return total
            total = lax.fori_loop(0, nx, along, jnp.zeros((chunk, lanes), jnp.float32))
            if counts[1] > 1:
                @pl.when(jnp.logical_not(has[1][0]))
                def _():
                    sum_out[y, pl.ds(z, chunk), :] = total
                    if (z + chunk) % half == 0:
                        s_copy(y, z // half).start()
        return 0
    lax.fori_loop(0, ny, last_row, 0)

    scale = 1.0 / (nx * counts[1])

    def finish(i, _):
        y, part = order(i // parts), i % parts
        places = [pl.ds(pl.multiple_of(part * half + z, PAD), chunk) for z in range(0, half, chunk)]
        if counts[1] > 1:
            @pl.when(has[1][0])
            def _():
                s_wait(y, part).wait_recv()
                @pl.when(has[1][1])
                def _():
                    for at in places:
                        sum_out[y, at, :] = sum_in[y, at, :] + speed[y, nx - 1, at, :]
                    s_copy(y, part).start()
        for at in places:
            below = sum_in[y, at, :]
            for x in range(nx):
                speed[y, x, at, :] = (speed[y, x, at, :] + below) * scale
        return 0
    lax.fori_loop(0, ny * parts, finish, 0)

    def drain(i, _):
        y = order(i)
        sent(last, y)
        if counts[1] > 1:
            @pl.when(has[1][1])
            def _():
                for part in range(parts):
                    s_copy(y, part).wait_send()
        return 0
    lax.fori_loop(0, ny, drain, 0)


def write(rows, sum_ref, end_ref, sum_hbm, end_hbm, sem):
    def copies(y):
        return (pltpu.make_async_copy(sum_ref.at[y], sum_hbm.at[y], sem.at[0, y]),
                pltpu.make_async_copy(end_ref.at[y], end_hbm.at[y], sem.at[1, y]))

    for y in range(rows):
        for copy in copies(y):
            copy.start()
    for y in range(rows):
        for copy in copies(y):
            copy.wait()


def solution(mesh):
    counts = tuple(mesh.shape[axis] for axis in AXES)

    def on_device(pressure, earlier, speed_square):
        block = pressure.shape
        ny, nx, nz, lanes = block
        f32 = jnp.float32
        anywhere = pl.BlockSpec(memory_space=pl.ANY)
        inside = pl.BlockSpec(memory_space=pltpu.VMEM)
        dma = pltpu.SemaphoreType.DMA
        column_sum, pressure_end = pl.pallas_call(
            functools.partial(kernel, counts, block),
            out_shape=[pltpu.VMEM(block, f32)] * 2,
            in_specs=[anywhere] * 3,
            out_specs=[inside] * 2,
            scratch_shapes=[
                pltpu.VMEM((2, ny + 2, nx + 2, nz + 2 * PAD, lanes), f32),
                pltpu.VMEM((2, 2, ny, nx, lanes), f32),
                pltpu.VMEM((2, 2, ny, nx, lanes), f32),
                pltpu.VMEM((ny, nz, lanes), f32),
                pltpu.VMEM((ny, nz, lanes), f32),
                dma((3, ny)),
                dma((2, 2, ny)), dma((2, 2, ny)),
                dma((2, 2)), dma((2, 2)),
                dma((2, 2, ny)), dma((2, 2, ny)),
                dma((ny, pieces(nz))), dma((ny, pieces(nz))),
            ],
            compiler_params=pltpu.CompilerParams(
                collective_id=0, has_side_effects=True, vmem_limit_bytes=40 * 1024 * 1024
            ),
        )(pressure, earlier, speed_square)
        return pl.pallas_call(
            functools.partial(write, ny),
            out_shape=[jax.ShapeDtypeStruct(block, f32)] * 2,
            in_specs=[inside] * 2,
            out_specs=[anywhere] * 2,
            scratch_shapes=[dma((2, ny))],
            compiler_params=pltpu.CompilerParams(vmem_limit_bytes=1024 * 1024),
        )(column_sum, pressure_end)

    spec = P("rows", "cols", "slabs", None)
    return jax.shard_map(
        on_device, mesh=mesh, in_specs=(spec, spec, spec), out_specs=(spec, spec), check_vma=False
    )
```
